32 devices in a mesh: expert: 4 (over y, x), shard: 8 (over z, core).
Axes of the slice: x: 2, y: 2, z: 4, core: 2. Of those that a mesh axis runs over, the one named last changes fastest.
Arguments:
- master_gate: float32 [64, 2048, 1408], P('expert', 'shard'), may hold values from -0.1875 to 0.1875
- master_up: float32 [64, 2048, 1408], P('expert', 'shard'), may hold values from -0.1875 to 0.1875
- master_down: float32 [64, 1408, 2048], P('expert', None, 'shard'), may hold values from -0.21875 to 0.21875
- router_weight: float32 [2048, 64], P('shard', 'expert'), may hold values from -0.125 to 0.125
- router_gain: float32 [2048], P('shard'), may hold values from 0.25 to 1.75
Outputs:
- final_gate: bfloat16 [64, 2048, 1408], P('expert', None, 'shard')
- final_up: bfloat16 [64, 2048, 1408], P('expert', None, 'shard')
- final_down: bfloat16 [64, 1408, 2048], P('expert', 'shard')
- scale_gate: float32 [64, 1408], P('expert', 'shard')
- scale_up: float32 [64, 1408], P('expert', 'shard')
- scale_down: float32 [64, 1408], P('expert', 'shard')
- serve_router: bfloat16 [2048, 64], replicated
The draws below stay inside these ranges and needn't reach their ends.
All inputs are finite; a program needn't handle non-finite values. Where the reference program divides by a largest or mean magnitude, that divisor is 1e-20 or more.
Results may differ from the reference program's by a relative error of at most 0.001.
Values may be sent and summed in bfloat16 or wider, within the bound.
A program may use at most 256 MiB of HBM per device.

```python
import jax
import jax.numpy as jnp

EXPERTS = 64
D_MODEL = 2048
D_EXPERT = 1408


def with_spikes(drawn, stream_key, source, target, shards_of, factor):
    owner, partner = [(jnp.arange(drawn.shape[position]) // (drawn.shape[position] // shards_of)).reshape([-1 if axis == position else 1 for axis in range(drawn.ndim)]) for position in (source, target)]
    chosen = jax.random.permutation(stream_key, shards_of)[partner]
    strong = (owner == chosen) | (owner == (partner + shards_of // 2) % shards_of)
    return jnp.where(strong, factor * drawn, drawn)


def shard_levels(rng, dims, cuts, low, largest):
    def one(axis_at, blocks):
        heights = jax.random.uniform(jax.random.fold_in(jax.random.fold_in(rng, 6), axis_at), (blocks,), jnp.float32, low / len(cuts), largest / len(cuts))
        return jnp.repeat(jnp.exp(heights), dims[axis_at] // blocks).reshape((-1,) + (1,) * (len(dims) - axis_at - 1))

    gain = one(*cuts[0])
    for cut in cuts[1:]:
        gain = gain * one(*cut)
    return gain


def bell_draw(key, shape, scale, bound, cuts=(), kind=jnp.bfloat16):
    values = jax.random.normal(key, shape, jnp.float32) * scale
    if len(cuts) > 0:
        values = shard_levels(key, shape, cuts, -0.22, 0.18) * values
    return jnp.clip(values, min=-bound, max=bound).astype(kind)


def bell_draw_with(stream_key, shape, scale, most, split, heavy, held_as=jnp.bfloat16):
    array = scale * jax.random.normal(stream_key, shape, jnp.float32)
    if split:
        array = array * shard_levels(stream_key, shape, split, -0.22, 0.18)
    return jnp.clip(with_spikes(array, jax.random.fold_in(stream_key, 3), *heavy), -most, most).astype(held_as)


def setup_inputs(seed: int = 0) -> dict:
    key_list = jax.random.split(jax.random.key(seed), 6)
    master_gate = bell_draw_with(key_list[0], (EXPERTS, D_MODEL, D_EXPERT), D_MODEL ** -0.5, 0.1875, ((0, 4), (1, 8)), (1, 2, 8, 2.0), jnp.float32)
    master_up = bell_draw_with(key_list[1], (EXPERTS, D_MODEL, D_EXPERT), D_MODEL ** -0.5, 0.1875, ((0, 4), (1, 8)), (1, 2, 8, 2.0), jnp.float32)
    master_down = bell_draw_with(key_list[2], (EXPERTS, D_EXPERT, D_MODEL), D_EXPERT ** -0.5, 0.21875, ((0, 4), (2, 8)), (2, 1, 8, 2.0), jnp.float32)
    router_weight = bell_draw(key_list[3], (D_MODEL, EXPERTS), D_MODEL ** -0.5, 0.125, ((0, 8), (1, 4)), jnp.float32)
    router_gain = jnp.clip(1.0 + 0.15 * jax.random.normal(key_list[4], (D_MODEL,), jnp.float32), 0.25, 1.75)
    return dict(master_gate=master_gate, master_up=master_up, master_down=master_down, router_weight=router_weight, router_gain=router_gain)


def reference(master_gate, master_up, master_down, router_weight, router_gain):
    scale_gate = jnp.max(jnp.abs(master_gate), axis=1)
    final_gate = (master_gate / jnp.expand_dims(scale_gate, 1)).astype(jnp.bfloat16)
    scale_up = jnp.max(jnp.abs(master_up), axis=1)
    final_up = (master_up / jnp.expand_dims(scale_up, 1)).astype(jnp.bfloat16)
    scale_down = jnp.max(jnp.abs(master_down), axis=2)
    final_down = (master_down / jnp.expand_dims(scale_down, 2)).astype(jnp.bfloat16)
    serve_router = (router_weight * router_gain[:, None]).astype(jnp.bfloat16)
    return final_gate, final_up, final_down, scale_gate, scale_up, scale_down, serve_router
```

```python
import functools

import jax
import jax.numpy as jnp
from jax import lax
from jax.experimental import pallas as pl
from jax.experimental.pallas import tpu as pltpu
from jax.sharding import PartitionSpec as P

MESH = pl.DeviceIdType.MESH
LANES = 128
PAIR = 2
CORES = 2
HELD_SHARE = 6
LEAD = 2


def across(n, me):
    half = n // 2
    return [(1 - me // half) * half + lax.rem(me, CORES) + CORES * q for q in range(half // CORES)]


def kernel(
    n, groups_of_experts, gate, up, down, weight, gain,
    out_gate, out_up, out_down, scales, router, later,
    wide_max, tall_max, wide, tall, turned, column, stage, local, got, kept, part, rows,
    load_max, load_bulk, msg_send, msg_recv, bulk_send, bulk_recv, own_sem, router_sem, later_sem,
    first, first_send, first_recv, turn,
):
    me = lax.axis_index("shard")
    team = lax.axis_index("expert")
    experts, depth, inner = gate.shape
    block = inner // n
    per_array = experts // PAIR
    total = 3 * per_array
    direct = LEAD * PAIR
    wide_groups = 2 * per_array
    bits = n.bit_length() - 1
    cross, share, last = bits - 1, bits, bits + 1
    steps = bits + 2
    ins, outs = (gate, up, down), (out_gate, out_up, out_down)
    core = lax.rem(me, CORES)
    half = n // 2
    held = later.shape[0]
    first_held = 3 * experts - held

    def partner(step):
        size = {share: CORES, last: 1}.get(step, 2**step)
        return me + (1 - 2 * lax.rem(me // size, 2)) * size

    def crosses(group):
        return lax.rem(me // CORES, 2) == lax.rem(group, 2)

    barrier = pltpu.get_barrier_semaphore()
    for d in range(1, n):
        pl.semaphore_signal(barrier, inc=1, device_id={"shard": lax.rem(me + d, n)}, device_id_type=MESH)
    for d in range(1, groups_of_experts):
        pl.semaphore_signal(
            barrier, inc=1, device_id={"expert": lax.rem(team + d, groups_of_experts)}, device_id_type=MESH
        )

    def load(group, wide_buf, tall_buf, sem, act):
        for m in range(3):

            @pl.when(group // per_array == m)
            def _():
                first = lax.rem(group, per_array) * PAIR
                act(pltpu.make_async_copy(ins[m].at[pl.ds(first, PAIR)], tall_buf if m == 2 else wide_buf, sem))

    load(0, wide, tall, load_bulk, lambda c: c.start())
    load(1, wide_max, tall_max, load_max, lambda c: c.start())

    def first_max(source, j, chunk):
        for b in range(inner // LANES):
            lanes = pl.ds(b * LANES, LANES)
            first[me, chunk, :, lanes] = jnp.max(jnp.abs(source[j, :, lanes]), axis=0, keepdims=True)

    def first_message(k, d):
        own = first.at[me, pl.ds(k, 1 if k == 0 else direct - 1)]
        return pltpu.make_async_remote_copy(
            own, own, first_send.at[k], first_recv.at[k],
            device_id={"shard": lax.rem(me + d, n)}, device_id_type=MESH,
        )

    def first_bytes(k):
        return first.at[pl.ds(0, n - 1), pl.ds(k, 1 if k == 0 else direct - 1)]

    load(0, wide, tall, load_bulk, lambda c: c.wait())
    first_max(wide, 0, 0)
    pl.semaphore_wait(barrier, n + groups_of_experts - 2)
    for d in range(1, n):
        first_message(0, d).start()
    for j in range(1, PAIR):
        first_max(wide, j, j)
    load(1, wide_max, tall_max, load_max, lambda c: c.wait())
    for j in range(PAIR):
        first_max(wide_max, j, PAIR + j)
    load(LEAD, wide_max, tall_max, load_max, lambda c: c.start())
    for d in range(1, n):
        first_message(1, d).start()

    team_rows = pl.ds(pl.multiple_of(team * part.shape[0], part.shape[0]), part.shape[0])
    my_columns = pl.ds(pl.multiple_of(me * depth, depth), depth)
    product = (weight[...] * gain[...]).astype(jnp.bfloat16)
    part[...] = product
    rows[team_rows, my_columns] = product
    for d in range(1, n):
        pltpu.make_async_remote_copy(
            part, rows.at[team_rows, my_columns], router_sem.at[0], router_sem.at[1],
            device_id={"shard": lax.rem(me + d, n)}, device_id_type=MESH,
        ).start()
    router_bytes = rows.at[pl.ds(0, part.shape[0]), pl.ds(0, (n - 1) * depth)]
    team_bytes = rows.at[pl.ds(0, (groups_of_experts - 1) * part.shape[0])]

    def message(step, group):
        source = local.at[group * PAIR + 1 - core] if step == 0 else kept.at[step, group]
        return pltpu.make_async_remote_copy(
            source, got.at[step, group], msg_send.at[step, group], msg_recv.at[step, group],
            device_id={"shard": partner(step)}, device_id_type=MESH,
        )

    def local_max(group):
        load(group, wide_max, tall_max, load_max, lambda c: c.wait())

        @pl.when(group < wide_groups)
        def _():
            for j in range(PAIR):
                for b in range(inner // LANES):
                    lanes = pl.ds(b * LANES, LANES)
                    local[group * PAIR + j, :, lanes] = jnp.max(jnp.abs(wide_max[j, :, lanes]), axis=0, keepdims=True)

        @pl.when(group >= wide_groups)
        def _():
            for j in range(PAIR):
                for b in range(inner // LANES):
                    lanes = pl.ds(b * LANES, LANES)
                    most = jnp.abs(tall_max[j, lanes, pl.ds(0, LANES)])
                    for h in range(1, depth // LANES):
                        most = jnp.maximum(most, jnp.abs(tall_max[j, lanes, pl.ds(h * LANES, LANES)]))
                    local[group * PAIR + j, :, lanes] = jnp.max(most.T, axis=0, keepdims=True)

        @pl.when(group + 1 < total)
        def _():
            load(group + 1, wide_max, tall_max, load_max, lambda c: c.start())

        message(0, group).start()

    def reduce_step(step, group):
        if step < share:
            message(step - 1, group).wait_recv()
            held = local[group * PAIR + core] if step == 1 else kept[step - 1, group]
            kept[step, group] = jnp.maximum(held, got[step - 1, group])
            if step < cross:
                message(step, group).start()
                return

        @pl.when(crosses(group))
        def _():
            if step == share:
                message(cross, group).wait_recv()
                kept[share, group] = jnp.maximum(kept[cross, group], got[cross, group])
            if step == last:
                kept[last, group] = kept[share, group]
            else:
                message(step, group).start()

        if step == last:

            @pl.when(jnp.logical_not(crosses(group)))
            def _():
                message(share, group).wait_recv()
                kept[last, group] = got[share, group]

            scales[group * PAIR + core] = kept[last, group]
            message(last, group).start()

    def normalise(j, source, chunk, p):
        part_rows = pl.ds(p * block if isinstance(p, int) else pl.multiple_of(p * block, 8), block)
        for h in range(depth // LANES):
            lanes = pl.ds(h * LANES, LANES)
            x = source[part_rows, lanes] if j is None else source[j, part_rows, lanes]
            stage[chunk, p, :, lanes] = (x / column[part_rows]).astype(jnp.bfloat16)

    def spread(chunk):
        for b in range(inner // LANES):
            lanes = pl.ds(b * LANES, LANES)
            column[lanes] = jnp.broadcast_to(scales[chunk, :, lanes], (LANES, LANES)).T

    def turn_over(j):
        for b in range(inner // LANES):
            lanes = pl.ds(b * LANES, LANES)
            for h in range(depth // LANES):
                part = pl.ds(h * LANES, LANES)
                turned[lanes, part] = wide[j, part, lanes].T

    def keep(chunk, m):
        pltpu.make_async_copy(
            stage.at[chunk, me], outs[m].at[chunk - m * experts, :, my_columns], own_sem.at[m]
        ).start()

    def first_bulk(chunk):
        j = lax.rem(chunk, PAIR)

        @pl.when((chunk > 0) & (j == 0))
        def _():
            load(chunk // PAIR, wide, tall, load_bulk, lambda c: c.wait())

        turn_over(j)
        for k in range(2):

            @pl.when(chunk == k)
            def _():
                pltpu.make_async_copy(first_bytes(k), first_bytes(k), first_recv.at[k]).wait()

        for b in range(inner // LANES):
            lanes = pl.ds(b * LANES, LANES)
            scales[chunk, :, lanes] = jnp.max(first[:, chunk, :, lanes], axis=0)
        spread(chunk)
        for d in range(n):
            p = lax.rem(me + half + d, n)
            normalise(None, turned, chunk, p)
            if d == half:
                keep(chunk, 0)
            else:
                send(chunk, p, 0)

        @pl.when(j == PAIR - 1)
        def _():
            load((chunk + 1) // PAIR, wide, tall, load_bulk, lambda c: c.start())

    def send(chunk, p, m):
        s = m
        if m == 2:
            s = jnp.where(chunk >= first_held, jnp.where(chunk == 3 * experts - 1, 4, 3), 2)
        pltpu.make_async_remote_copy(
            stage.at[chunk, p], outs[m].at[chunk - m * experts, :, my_columns], bulk_send.at[s], bulk_recv.at[s],
            device_id={"shard": p}, device_id_type=MESH,
        ).start()

    def bulk(group):
        message(last, group).wait_recv()
        scales[group * PAIR + 1 - core] = got[last, group]

        load(group, wide, tall, load_bulk, lambda c: c.wait())

        @pl.loop(0, PAIR)
        def _(j):
            chunk = group * PAIR + j
            spread(chunk)

            @pl.when(group < wide_groups)
            def _():
                turn_over(j)
                for p in range(n):
                    normalise(None, turned, chunk, p)

            @pl.when(group >= wide_groups)
            def _():
                for p in range(n):
                    normalise(j, tall, chunk, p)

            for m in range(3):

                @pl.when(group // per_array == m)
                def _():
                    for d in range(n):
                        p = lax.rem(me + n // 2 + d, n)
                        if d == n // 2:
                            keep(chunk, m)
                        elif m < 2 or d % CORES:
                            send(chunk, p, m)
                        else:
                            hold = (chunk >= first_held) & (p // half != me // half)

                            @pl.when(jnp.logical_not(hold))
                            def _():
                                send(chunk, p, m)

                            @pl.when(hold & (core == 0))
                            def _():
                                pltpu.make_async_copy(
                                    stage.at[chunk, p], later.at[chunk - first_held, lax.rem(p, half) // CORES], later_sem
                                ).start()

        @pl.when(group + 1 < total)
        def _():
            load(group + 1, wide, tall, load_bulk, lambda c: c.start())

    @pl.loop(LEAD, total + steps)
    def _(t):
        for step in reversed(range(1, steps)):

            @pl.when((t >= step + LEAD) & (t < total + step))
            def _():
                reduce_step(step, t - step)

        @pl.when(t < total)
        def _():
            local_max(t)

        @pl.when(t == LEAD + 1)
        def _():
            pltpu.make_async_copy(router_bytes, router_bytes, router_sem.at[1]).wait()
            for d in range(1, groups_of_experts):
                pltpu.make_async_remote_copy(
                    rows.at[team_rows], rows.at[team_rows], router_sem.at[2], router_sem.at[3],
                    device_id={"expert": lax.rem(team + d, groups_of_experts)}, device_id_type=MESH,
                ).start()

        @pl.when((t > LEAD) & (t <= LEAD + direct))
        def _():
            first_bulk(t - LEAD - 1)

        @pl.when(t >= LEAD + steps)
        def _():
            bulk(t - steps)

    def done(sems, s, m, count, width):
        moved = outs[m].at[pl.ds(0, count), :, pl.ds(0, width * depth)]
        pltpu.make_async_copy(moved, moved, sems.at[s]).wait()

    def done_first(sems, narrow):
        for m in range(3):
            done(sems, m, m, experts - held if m == 2 else experts, n - 1)
        done(sems, 3, 2, held - 1, n - 1 - narrow)

    @pl.when(core == 0)
    def _():
        done_first(bulk_send, half // CORES)
        for q in range(half // CORES):
            pl.semaphore_signal(
                turn, inc=1, device_id={"shard": me // half * half + CORES * q + 1}, device_id_type=MESH
            )
        done(bulk_send, 4, 2, 1, n - 1 - half // CORES)

    @pl.when(core > 0)
    def _():
        pl.semaphore_wait(turn, half // CORES)

        @pl.loop(first_held, 3 * experts)
        def _(chunk):
            for p in across(n, me):
                send(chunk, p, 2)

    pltpu.make_async_copy(router_bytes, router_bytes, router_sem.at[0]).wait()
    for s in (2, 3):
        pltpu.make_async_copy(team_bytes, team_bytes, router_sem.at[s]).wait()
    router[...] = rows[...]

    @pl.loop(LEAD, total)
    def _(group):
        for step in range(steps):
            if step in (cross, share):

                @pl.when(crosses(group))
                def _():
                    message(step, group).wait_send()
            else:
                message(step, group).wait_send()

    for k in range(2):
        pltpu.make_async_copy(first_bytes(k), first_bytes(k), first_send.at[k]).wait()

    for m in range(3):
        own = outs[m].at[:, :, pl.ds(0, depth)]
        pltpu.make_async_copy(own, own, own_sem.at[m]).wait()

    @pl.when(core == 0)
    def _():
        pltpu.make_async_copy(later, later, later_sem).wait()
        done_first(bulk_recv, half // CORES)
        done(bulk_recv, 4, 2, 1, n - 1 - half // CORES)

    @pl.when(core > 0)
    def _():
        for sems in (bulk_send, bulk_recv):
            done_first(sems, 0)
            done(sems, 4, 2, 1, n - 1)


def place(
    gate, up, down, router, out_gate, out_up, out_down, out_router, token,
    buffer, router_buffer, loads, stores, router_sem,
):
    ins, outs = (gate, up, down), (out_gate, out_up, out_down)
    experts = gate.shape[0]

    def load(m, e):
        chunk = m * experts + e
        return pltpu.make_async_copy(ins[m].at[e], buffer.at[chunk], loads.at[chunk])

    for m in range(3):

        @pl.loop(0, experts)
        def _(e):
            load(m, e).start()

    pltpu.make_async_copy(router, router_buffer, router_sem).start()
    for m in range(3):

        @pl.loop(0, experts)
        def _(e):
            load(m, e).wait()
            pltpu.make_async_copy(buffer.at[m * experts + e], outs[m].at[e], stores.at[m]).start()

    pltpu.make_async_copy(router, router_buffer, router_sem).wait()
    pltpu.make_async_copy(router_buffer, out_router, router_sem).start()
    token[...] = jnp.zeros_like(token)
    for m in range(3):
        pltpu.make_async_copy(outs[m], outs[m], stores.at[m]).wait()
    pltpu.make_async_copy(router_buffer, out_router, router_sem).wait()


def finish(n, later, token, late, send_sem, recv_sem):
    me = lax.axis_index("shard")
    held, others = later.shape[:2]

    @pl.when(lax.rem(me, CORES) == 0)
    def _():
        barrier = pltpu.get_barrier_semaphore()
        for p in across(n, me):
            pl.semaphore_signal(barrier, inc=1, device_id={"shard": p}, device_id_type=MESH)
        pl.semaphore_wait(barrier, others)

        @pl.loop(0, held)
        def _(i):
            for q, p in enumerate(across(n, me)):
                pltpu.make_async_remote_copy(
                    later.at[i, q], late.at[i, lax.rem(me, n // 2) // CORES], send_sem, recv_sem,
                    device_id={"shard": p}, device_id_type=MESH,
                ).start()

        pltpu.make_async_copy(late, late, send_sem).wait()
        pltpu.make_async_copy(late, late, recv_sem).wait()


def patch(n, late, down, out_down, buffer, loads, store):
    me = lax.axis_index("shard")
    held, others, block, depth = late.shape
    first = down.shape[0] - held

    @pl.when(lax.rem(me, CORES) == 0)
    def _():
        for i in range(held):
            for q in range(others):
                pltpu.make_async_copy(late.at[i, q], buffer.at[i, q], loads.at[i, q]).start()
        for i in range(held):
            for q, p in enumerate(across(n, me)):
                pltpu.make_async_copy(late.at[i, q], buffer.at[i, q], loads.at[i, q]).wait()
                columns = pl.ds(pl.multiple_of(p * depth, depth), depth)
                pltpu.make_async_copy(buffer.at[i, q], out_down.at[first + i, :, columns], store).start()
        pltpu.make_async_copy(late, late, store).wait()


def plain(master_gate, master_up, master_down, router_weight, router_gain):
    scale_gate, scale_up, scale_down = lax.pmax(
        (
            jnp.max(jnp.abs(master_gate), axis=1),
            jnp.max(jnp.abs(master_up), axis=1),
            jnp.max(jnp.abs(master_down), axis=2),
        ),
        "shard",
    )
    narrow_gate, narrow_up, narrow_down = (
        (master_gate / jnp.expand_dims(scale_gate, 1)).astype(jnp.bfloat16),
        (master_up / jnp.expand_dims(scale_up, 1)).astype(jnp.bfloat16),
        (master_down / jnp.expand_dims(scale_down, 2)).astype(jnp.bfloat16),
    )
    final_gate, final_up = (
        lax.all_to_all(narrow_gate, "shard", split_axis=2, concat_axis=1, tiled=True),
        lax.all_to_all(narrow_up, "shard", split_axis=2, concat_axis=1, tiled=True),
    )
    final_down = lax.all_to_all(narrow_down, "shard", split_axis=1, concat_axis=2, tiled=True)
    scale_gate = lax.dynamic_slice_in_dim(
        scale_gate, lax.axis_index("shard") * final_gate.shape[2], final_gate.shape[2], axis=1
    )
    scale_up = lax.dynamic_slice_in_dim(
        scale_up, lax.axis_index("shard") * final_up.shape[2], final_up.shape[2], axis=1
    )
    scale_down = lax.dynamic_slice_in_dim(
        scale_down, lax.axis_index("shard") * final_down.shape[1], final_down.shape[1], axis=1
    )
    part_router = (router_weight * router_gain[:, None]).astype(jnp.bfloat16)
    row_router = lax.all_gather(part_router, "shard", axis=0, tiled=True)
    serve_router = lax.all_gather(row_router, "expert", axis=1, tiled=True)
    return (final_gate, final_up, final_down, scale_gate, scale_up, scale_down, serve_router)


def solution(mesh):
    n, teams = mesh.shape["shard"], mesh.shape["expert"]

    def body(master_gate, master_up, master_down, router_weight, router_gain):
        experts, depth, inner = master_gate.shape
        block = inner // n
        chunks = 3 * experts
        groups = chunks // PAIR
        steps = n.bit_length() + 1
        columns = router_weight.shape[1]
        fits = depth % LANES == 0 and inner % LANES == 0 and block % 8 == 0
        if n < 8 or n & (n - 1) or experts < (LEAD + 1) * PAIR or experts % PAIR or not fits:
            return plain(master_gate, master_up, master_down, router_weight, router_gain)
        f32, bf16 = jnp.float32, jnp.bfloat16
        dma = pltpu.SemaphoreType.DMA
        final = jax.ShapeDtypeStruct((experts, block, n * depth), bf16)
        hbm, vmem = pl.BlockSpec(memory_space=pl.ANY), pl.BlockSpec(memory_space=pltpu.VMEM)
        held = chunks // HELD_SHARE
        others = n // 2 // CORES
        pieces = jax.ShapeDtypeStruct((held, others, block, depth), bf16)
        gate, up, down, scales, router, later = pl.pallas_call(
            functools.partial(kernel, n, teams),
            out_shape=(
                final, final, final,
                jax.ShapeDtypeStruct((chunks, 1, inner), f32),
                jax.ShapeDtypeStruct((teams * columns, n * depth), bf16),
                pieces,
            ),
            in_specs=[hbm, hbm, hbm, vmem, vmem],
            out_specs=(hbm, hbm, hbm, vmem, vmem, hbm),
            scratch_shapes=[
                pltpu.VMEM((PAIR, depth, inner), f32),
                pltpu.VMEM((PAIR, inner, depth), f32),
                pltpu.VMEM((PAIR, depth, inner), f32),
                pltpu.VMEM((PAIR, inner, depth), f32),
                pltpu.VMEM((inner, depth), f32),
                pltpu.VMEM((inner, LANES), f32),
                pltpu.VMEM((chunks, n, block, depth), bf16),
                pltpu.VMEM((chunks, 1, inner), f32),
                pltpu.VMEM((steps, groups, 1, inner), f32),
                pltpu.VMEM((steps, groups, 1, inner), f32),
                pltpu.VMEM((columns, depth), bf16),
                pltpu.VMEM((teams * columns, n * depth), bf16),
                dma, dma,
                dma((steps, groups)), dma((steps, groups)),
                dma((5,)), dma((5,)), dma((3,)), dma((4,)), dma,
                pltpu.VMEM((n, LEAD * PAIR, 1, inner), f32), dma((2,)), dma((2,)), pltpu.SemaphoreType.REGULAR,
            ],
            compiler_params=pltpu.CompilerParams(
                collective_id=0, has_side_effects=True, vmem_limit_bytes=62 * 1024 * 1024
            ),
        )(master_gate, master_up, master_down, router_weight.T, router_gain[None, :])
        mine = lax.dynamic_slice_in_dim(
            scales.reshape(3, experts, inner), lax.axis_index("shard") * block, block, axis=2
        )
        gate, up, down, router, token = pl.pallas_call(
            place,
            out_shape=(
                final, final, final,
                jax.ShapeDtypeStruct(router.shape, bf16),
                jax.ShapeDtypeStruct((8, LANES), f32),
            ),
            in_specs=[hbm, hbm, hbm, hbm],
            out_specs=(hbm, hbm, hbm, hbm, vmem),
            scratch_shapes=[
                pltpu.VMEM((chunks, block, n * depth), bf16),
                pltpu.VMEM(router.shape, bf16),
                dma((chunks,)), dma((3,)), dma,
            ],
            compiler_params=pltpu.CompilerParams(vmem_limit_bytes=62 * 1024 * 1024),
        )(gate, up, down, router)
        token, scale_gate, scale_up, scale_down = lax.optimization_barrier((token, mine[0], mine[1], mine[2]))
        late = pl.pallas_call(
            functools.partial(finish, n),
            out_shape=pieces,
            in_specs=[hbm, hbm],
            out_specs=hbm,
            scratch_shapes=[dma, dma],
            compiler_params=pltpu.CompilerParams(
                collective_id=1, has_side_effects=True, vmem_limit_bytes=62 * 1024 * 1024
            ),
        )(later, token)
        down = pl.pallas_call(
            functools.partial(patch, n),
            out_shape=final,
            in_specs=[hbm, hbm],
            out_specs=hbm,
            scratch_shapes=[pltpu.VMEM(pieces.shape, bf16), dma((held, others)), dma],
            input_output_aliases={1: 0},
            compiler_params=pltpu.CompilerParams(vmem_limit_bytes=62 * 1024 * 1024),
        )(late, down)
        return (gate.swapaxes(1, 2), up.swapaxes(1, 2), down, scale_gate, scale_up, scale_down, router.T)

    return jax.shard_map(
        body,
        mesh=mesh,
        in_specs=(
            P("expert", "shard", None),
            P("expert", "shard", None),
            P("expert", None, "shard"),
            P("shard", "expert"),
            P("shard"),
        ),
        out_specs=(
            P("expert", None, "shard"),
            P("expert", None, "shard"),
            P("expert", "shard", None),
            P("expert", "shard"),
            P("expert", "shard"),
            P("expert", "shard"),
            P(),
        ),
        check_vma=False,
    )
```

```python
import functools

import jax
import jax.numpy as jnp
from jax import lax
from jax.experimental import pallas as pl
from jax.experimental.pallas import tpu as pltpu
from jax.sharding import PartitionSpec as P

MESH = pl.DeviceIdType.MESH
LANES = 128
PAIR = 2
CORES = 2
HELD_SHARE = 5
EARLY = 2
LEAD = 2


def across(n, me):
    half = n // 2
    return [(1 - me // half) * half + lax.rem(me, CORES) + CORES * q for q in range(half // CORES)]


def other(me, offset):
    for bit in range(offset.bit_length()):
        if offset >> bit & 1:
            me = me + (1 - 2 * lax.rem(me // 2**bit, 2)) * 2**bit
    return me


def kernel(
    n, groups_of_experts, gate, up, down, weight, gain,
    out_gate, out_up, out_down, scales, router, later,
    wide_max, tall_max, wide, tall, turned, column, stage, local, got, kept, part, rows,
    load_max, load_bulk, msg_send, msg_recv, bulk_send, bulk_recv, own_sem, router_sem, later_sem,
    first, first_load, first_send, first_recv, turn,
):
    me = lax.axis_index("shard")
    team = lax.axis_index("expert")
    experts, depth, inner = gate.shape
    block = inner // n
    per_array = experts // PAIR
    total = 3 * per_array
    direct = LEAD * PAIR
    wide_groups = 2 * per_array
    bits = n.bit_length() - 1
    cross, share, last = bits - 1, bits, bits + 1
    steps = bits + 2
    ins, outs = (gate, up, down), (out_gate, out_up, out_down)
    core = lax.rem(me, CORES)
    half = n // 2
    held = later.shape[0]
    first_held = 3 * experts - held

    def partner(step):
        size = {share: CORES, last: 1}.get(step, 2**step)
        return me + (1 - 2 * lax.rem(me // size, 2)) * size

    far, near = list(range(half, n)), list(range(CORES, half))
    orders = (far + near + [1, 0], near + far + [1, 0])

    def crosses(group):
        return lax.rem(me // CORES, 2) == lax.rem(group, 2)

    barrier = pltpu.get_barrier_semaphore()
    for d in range(1, n):
        pl.semaphore_signal(barrier, inc=1, device_id={"shard": lax.rem(me + d, n)}, device_id_type=MESH)
    for d in range(1, groups_of_experts):
        pl.semaphore_signal(
            barrier, inc=1, device_id={"expert": lax.rem(team + d, groups_of_experts)}, device_id_type=MESH
        )

    def load(group, wide_buf, tall_buf, sem, act):
        for m in range(3):

            @pl.when(group // per_array == m)
            def _():
                first = lax.rem(group, per_array) * PAIR
                act(pltpu.make_async_copy(ins[m].at[pl.ds(first, PAIR)], tall_buf if m == 2 else wide_buf, sem))

    def load_first(part, sem):
        return pltpu.make_async_copy(gate.at[part], wide.at[part], sem)

    head, rest = pl.ds(0, 1), pl.ds(1, PAIR - 1)
    load_first(head, load_bulk).start()
    load_first(rest, first_load).start()
    load(1, wide_max, tall_max, load_max, lambda c: c.start())

    def first_max(source, j, chunk):
        for b in range(inner // LANES):
            lanes = pl.ds(b * LANES, LANES)
            first[me, chunk, :, lanes] = jnp.max(jnp.abs(source[j, :, lanes]), axis=0, keepdims=True)

    def first_message(k, d):
        own = first.at[me, pl.ds(k, 1 if k == 0 else direct - 1)]
        return pltpu.make_async_remote_copy(
            own, own, first_send.at[k], first_recv.at[k],
            device_id={"shard": lax.rem(me + d, n)}, device_id_type=MESH,
        )

    def first_bytes(k):
        return first.at[pl.ds(0, n - 1), pl.ds(k, 1 if k == 0 else direct - 1)]

    load_first(head, load_bulk).wait()
    first_max(wide, 0, 0)
    pl.semaphore_wait(barrier, n + groups_of_experts - 2)
    for d in range(1, n):
        first_message(0, d).start()
    load_first(rest, first_load).wait()
    for j in range(1, PAIR):
        first_max(wide, j, j)
    load(1, wide_max, tall_max, load_max, lambda c: c.wait())
    for j in range(PAIR):
        first_max(wide_max, j, PAIR + j)
    load(LEAD, wide_max, tall_max, load_max, lambda c: c.start())
    for d in range(1, n):
        first_message(1, d).start()

    team_rows = pl.ds(pl.multiple_of(team * part.shape[0], part.shape[0]), part.shape[0])
    my_columns = pl.ds(pl.multiple_of(me * depth, depth), depth)
    product = (weight[...] * gain[...]).astype(jnp.bfloat16)
    part[...] = product
    rows[team_rows, my_columns] = product
    for d in range(1, n):
        pltpu.make_async_remote_copy(
            part, rows.at[team_rows, my_columns], router_sem.at[0], router_sem.at[1],
            device_id={"shard": lax.rem(me + d, n)}, device_id_type=MESH,
        ).start()
    router_bytes = rows.at[pl.ds(0, part.shape[0]), pl.ds(0, (n - 1) * depth)]
    team_bytes = rows.at[pl.ds(0, (groups_of_experts - 1) * part.shape[0])]

    def message(step, group):
        source = local.at[group * PAIR + 1 - core] if step == 0 else kept.at[step, group]
        return pltpu.make_async_remote_copy(
            source, got.at[step, group], msg_send.at[step, group], msg_recv.at[step, group],
            device_id={"shard": partner(step)}, device_id_type=MESH,
        )

    def local_max(group):
        load(group, wide_max, tall_max, load_max, lambda c: c.wait())

        @pl.when(group < wide_groups)
        def _():
            for j in range(PAIR):
                for b in range(inner // LANES):
                    lanes = pl.ds(b * LANES, LANES)
                    local[group * PAIR + j, :, lanes] = jnp.max(jnp.abs(wide_max[j, :, lanes]), axis=0, keepdims=True)

        @pl.when(group >= wide_groups)
        def _():
            for j in range(PAIR):
                for b in range(inner // LANES):
                    lanes = pl.ds(b * LANES, LANES)
                    most = jnp.abs(tall_max[j, lanes, pl.ds(0, LANES)])
                    for h in range(1, depth // LANES):
                        most = jnp.maximum(most, jnp.abs(tall_max[j, lanes, pl.ds(h * LANES, LANES)]))
                    local[group * PAIR + j, :, lanes] = jnp.max(most.T, axis=0, keepdims=True)

        @pl.when(group + 1 < total)
        def _():
            load(group + 1, wide_max, tall_max, load_max, lambda c: c.start())

        message(0, group).start()

    def reduce_step(step, group):
        if step < share:
            message(step - 1, group).wait_recv()
            held = local[group * PAIR + core] if step == 1 else kept[step - 1, group]
            kept[step, group] = jnp.maximum(held, got[step - 1, group])
            if step < cross:
                message(step, group).start()
                return

        @pl.when(crosses(group))
        def _():
            if step == share:
                message(cross, group).wait_recv()
                kept[share, group] = jnp.maximum(kept[cross, group], got[cross, group])
            if step == last:
                kept[last, group] = kept[share, group]
            else:
                message(step, group).start()

        if step == last:

            @pl.when(jnp.logical_not(crosses(group)))
            def _():
                message(share, group).wait_recv()
                kept[last, group] = got[share, group]

            scales[group * PAIR + core] = kept[last, group]
            message(last, group).start()

    def normalise(j, source, chunk, p):
        part_rows = pl.ds(p * block if isinstance(p, int) else pl.multiple_of(p * block, 8), block)
        for h in range(depth // LANES):
            lanes = pl.ds(h * LANES, LANES)
            x = source[part_rows, lanes] if j is None else source[j, part_rows, lanes]
            stage[chunk, p, :, lanes] = (x / column[part_rows]).astype(jnp.bfloat16)

    def spread(chunk):
        for b in range(inner // LANES):
            lanes = pl.ds(b * LANES, LANES)
            column[lanes] = jnp.broadcast_to(scales[chunk, :, lanes], (LANES, LANES)).T

    def turn_over(j):
        for b in range(inner // LANES):
            lanes = pl.ds(b * LANES, LANES)
            for h in range(depth // LANES):
                part = pl.ds(h * LANES, LANES)
                turned[lanes, part] = wide[j, part, lanes].T

    def keep(chunk, m):
        pltpu.make_async_copy(
            stage.at[chunk, me], outs[m].at[chunk - m * experts, :, my_columns], own_sem.at[m]
        ).start()

    def first_bulk(chunk):
        j = lax.rem(chunk, PAIR)

        @pl.when((chunk > 0) & (j == 0))
        def _():
            load(chunk // PAIR, wide, tall, load_bulk, lambda c: c.wait())

        turn_over(j)
        for k in range(2):

            @pl.when(chunk == k)
            def _():
                pltpu.make_async_copy(first_bytes(k), first_bytes(k), first_recv.at[k]).wait()

        for b in range(inner // LANES):
            lanes = pl.ds(b * LANES, LANES)
            scales[chunk, :, lanes] = jnp.max(first[:, chunk, :, lanes], axis=0)
        spread(chunk)
        for c in range(CORES):

            @pl.when(core == c)
            def _():
                for offset in orders[c]:
                    p = other(me, offset)
                    normalise(None, turned, chunk, p)
                    if offset == 0:
                        keep(chunk, 0)
                    else:
                        send(chunk, p, 0)

        @pl.when(j == PAIR - 1)
        def _():
            load((chunk + 1) // PAIR, wide, tall, load_bulk, lambda c: c.start())

    def send(chunk, p, m):
        s = m
        if m == 2:
            s = jnp.where(chunk >= first_held, jnp.where(chunk == 3 * experts - 1, 4, 3), 2)
        pltpu.make_async_remote_copy(
            stage.at[chunk, p], outs[m].at[chunk - m * experts, :, my_columns], bulk_send.at[s], bulk_recv.at[s],
            device_id={"shard": p}, device_id_type=MESH,
        ).start()

    def deal(chunk, offset, m, c):
        p = other(me, offset)
        if offset == 0:
            keep(chunk, m)
        elif m < 2 or offset < half or offset % CORES:
            send(chunk, p, m)
        else:

            @pl.when(chunk < first_held)
            def _():
                send(chunk, p, m)

            if c == 0:

                @pl.when(chunk >= first_held)
                def _():
                    pltpu.make_async_copy(
                        stage.at[chunk, p], later.at[chunk - first_held, lax.rem(p, half) // CORES], later_sem
                    ).start()

    def bulk(group):
        message(last, group).wait_recv()
        scales[group * PAIR + 1 - core] = got[last, group]

        load(group, wide, tall, load_bulk, lambda c: c.wait())

        @pl.loop(0, PAIR)
        def _(j):
            chunk = group * PAIR + j
            spread(chunk)

            @pl.when(group < wide_groups)
            def _():
                turn_over(j)
                for p in range(n):
                    normalise(None, turned, chunk, p)

            @pl.when(group >= wide_groups)
            def _():
                for p in range(n):
                    normalise(j, tall, chunk, p)

            for m in range(3):

                @pl.when(group // per_array == m)
                def _():
                    for c in range(CORES):

                        @pl.when(core == c)
                        def _():
                            for offset in orders[c]:
                                deal(chunk, offset, m, c)

        @pl.when(group + 1 < total)
        def _():
            load(group + 1, wide, tall, load_bulk, lambda c: c.start())

    @pl.loop(LEAD, total + steps)
    def _(t):
        for step in reversed(range(1, steps)):

            @pl.when((t >= step + LEAD) & (t < total + step))
            def _():
                reduce_step(step, t - step)

        @pl.when((t > LEAD) & (t <= LEAD + direct))
        def _():
            first_bulk(t - LEAD - 1)

        @pl.when(t < total)
        def _():
            local_max(t)

        @pl.when(t == LEAD + 1)
        def _():
            pltpu.make_async_copy(router_bytes, router_bytes, router_sem.at[1]).wait()
            for d in range(1, groups_of_experts):
                pltpu.make_async_remote_copy(
                    rows.at[team_rows], rows.at[team_rows], router_sem.at[2], router_sem.at[3],
                    device_id={"expert": lax.rem(team + d, groups_of_experts)}, device_id_type=MESH,
                ).start()

        @pl.when(t >= LEAD + steps)
        def _():
            bulk(t - steps)

    def done(sems, s, m, count, width):
        moved = outs[m].at[pl.ds(0, count), :, pl.ds(0, width * depth)]
        pltpu.make_async_copy(moved, moved, sems.at[s]).wait()

    def done_first(sems, narrow):
        for m in range(3):
            done(sems, m, m, experts - held if m == 2 else experts, n - 1)
        done(sems, 3, 2, held - 1, n - 1 - narrow)

    @pl.when(core == 0)
    def _():
        done_first(bulk_send, half // CORES)
        done(bulk_send, 4, 2, 1, n - 1 - half // CORES)
        for q in range(half // CORES):
            pl.semaphore_signal(
                turn, inc=1, device_id={"shard": me // half * half + CORES * q + 1}, device_id_type=MESH
            )

    @pl.when(core > 0)
    def _():
        def send_held(chunk):
            for p in across(n, me):
                send(chunk, p, 2)

        pl.loop(first_held, first_held + EARLY)(send_held)
        pl.semaphore_wait(turn, half // CORES)
        pl.loop(first_held + EARLY, 3 * experts)(send_held)

    pltpu.make_async_copy(router_bytes, router_bytes, router_sem.at[0]).wait()
    for s in (2, 3):
        pltpu.make_async_copy(team_bytes, team_bytes, router_sem.at[s]).wait()
    router[...] = rows[...]

    @pl.loop(LEAD, total)
    def _(group):
        for step in range(steps):
            if step in (cross, share):

                @pl.when(crosses(group))
                def _():
                    message(step, group).wait_send()
            else:
                message(step, group).wait_send()

    for k in range(2):
        pltpu.make_async_copy(first_bytes(k), first_bytes(k), first_send.at[k]).wait()

    for m in range(3):
        own = outs[m].at[:, :, pl.ds(0, depth)]
        pltpu.make_async_copy(own, own, own_sem.at[m]).wait()

    @pl.when(core == 0)
    def _():
        pltpu.make_async_copy(later, later, later_sem).wait()
        done_first(bulk_recv, half // CORES)
        done(bulk_recv, 4, 2, 1, n - 1 - half // CORES)

    @pl.when(core > 0)
    def _():
        for sems in (bulk_send, bulk_recv):
            done_first(sems, 0)
            done(sems, 4, 2, 1, n - 1)


def place(
    gate, up, down, router, out_gate, out_up, out_down, out_router, token,
    buffer, router_buffer, loads, stores, router_sem,
):
    ins, outs = (gate, up, down), (out_gate, out_up, out_down)
    experts = gate.shape[0]

    def load(m, e):
        chunk = m * experts + e
        return pltpu.make_async_copy(ins[m].at[e], buffer.at[chunk], loads.at[chunk])

    for m in range(3):

        @pl.loop(0, experts)
        def _(e):
            load(m, e).start()

    pltpu.make_async_copy(router, router_buffer, router_sem).start()
    for m in range(3):

        @pl.loop(0, experts)
        def _(e):
            load(m, e).wait()
            pltpu.make_async_copy(buffer.at[m * experts + e], outs[m].at[e], stores.at[m]).start()

    pltpu.make_async_copy(router, router_buffer, router_sem).wait()
    pltpu.make_async_copy(router_buffer, out_router, router_sem).start()
    token[...] = jnp.zeros_like(token)
    for m in range(3):
        pltpu.make_async_copy(outs[m], outs[m], stores.at[m]).wait()
    pltpu.make_async_copy(router_buffer, out_router, router_sem).wait()


def finish(n, later, token, late, send_sem, recv_sem):
    me = lax.axis_index("shard")
    held, others = later.shape[:2]

    @pl.when(lax.rem(me, CORES) == 0)
    def _():
        barrier = pltpu.get_barrier_semaphore()
        for p in across(n, me):
            pl.semaphore_signal(barrier, inc=1, device_id={"shard": p}, device_id_type=MESH)
        pl.semaphore_wait(barrier, others)

        @pl.loop(0, held)
        def _(i):
            for q, p in enumerate(across(n, me)):
                pltpu.make_async_remote_copy(
                    later.at[i, q], late.at[i, lax.rem(me, n // 2) // CORES], send_sem, recv_sem,
                    device_id={"shard": p}, device_id_type=MESH,
                ).start()

        pltpu.make_async_copy(late, late, send_sem).wait()
        pltpu.make_async_copy(late, late, recv_sem).wait()


def patch(n, late, down, out_down, buffer, loads, store):
    me = lax.axis_index("shard")
    held, others, block, depth = late.shape
    first = down.shape[0] - held

    @pl.when(lax.rem(me, CORES) == 0)
    def _():
        for i in range(held):
            for q in range(others):
                pltpu.make_async_copy(late.at[i, q], buffer.at[i, q], loads.at[i, q]).start()
        for i in range(held):
            for q, p in enumerate(across(n, me)):
                pltpu.make_async_copy(late.at[i, q], buffer.at[i, q], loads.at[i, q]).wait()
                columns = pl.ds(pl.multiple_of(p * depth, depth), depth)
                pltpu.make_async_copy(buffer.at[i, q], out_down.at[first + i, :, columns], store).start()
        pltpu.make_async_copy(late, late, store).wait()


def plain(master_gate, master_up, master_down, router_weight, router_gain):
    scale_gate, scale_up, scale_down = lax.pmax(
        (
            jnp.max(jnp.abs(master_gate), axis=1),
            jnp.max(jnp.abs(master_up), axis=1),
            jnp.max(jnp.abs(master_down), axis=2),
        ),
        "shard",
    )
    narrow_gate, narrow_up, narrow_down = (
        (master_gate / jnp.expand_dims(scale_gate, 1)).astype(jnp.bfloat16),
        (master_up / jnp.expand_dims(scale_up, 1)).astype(jnp.bfloat16),
        (master_down / jnp.expand_dims(scale_down, 2)).astype(jnp.bfloat16),
    )
    final_gate, final_up = (
        lax.all_to_all(narrow_gate, "shard", split_axis=2, concat_axis=1, tiled=True),
        lax.all_to_all(narrow_up, "shard", split_axis=2, concat_axis=1, tiled=True),
    )
    final_down = lax.all_to_all(narrow_down, "shard", split_axis=1, concat_axis=2, tiled=True)
    scale_gate = lax.dynamic_slice_in_dim(
        scale_gate, lax.axis_index("shard") * final_gate.shape[2], final_gate.shape[2], axis=1
    )
    scale_up = lax.dynamic_slice_in_dim(
        scale_up, lax.axis_index("shard") * final_up.shape[2], final_up.shape[2], axis=1
    )
    scale_down = lax.dynamic_slice_in_dim(
        scale_down, lax.axis_index("shard") * final_down.shape[1], final_down.shape[1], axis=1
    )
    part_router = (router_weight * router_gain[:, None]).astype(jnp.bfloat16)
    row_router = lax.all_gather(part_router, "shard", axis=0, tiled=True)
    serve_router = lax.all_gather(row_router, "expert", axis=1, tiled=True)
    return (final_gate, final_up, final_down, scale_gate, scale_up, scale_down, serve_router)


def solution(mesh):
    n, teams = mesh.shape["shard"], mesh.shape["expert"]

    def body(master_gate, master_up, master_down, router_weight, router_gain):
        experts, depth, inner = master_gate.shape
        block = inner // n
        chunks = 3 * experts
        groups = chunks // PAIR
        steps = n.bit_length() + 1
        columns = router_weight.shape[1]
        fits = depth % LANES == 0 and inner % LANES == 0 and block % 8 == 0
        if n < 8 or n & (n - 1) or experts < (LEAD + 1) * PAIR or experts % PAIR or not fits:
            return plain(master_gate, master_up, master_down, router_weight, router_gain)
        f32, bf16 = jnp.float32, jnp.bfloat16
        dma = pltpu.SemaphoreType.DMA
        final = jax.ShapeDtypeStruct((experts, block, n * depth), bf16)
        hbm, vmem = pl.BlockSpec(memory_space=pl.ANY), pl.BlockSpec(memory_space=pltpu.VMEM)
        held = chunks // HELD_SHARE
        others = n // 2 // CORES
        pieces = jax.ShapeDtypeStruct((held, others, block, depth), bf16)
        gate, up, down, scales, router, later = pl.pallas_call(
            functools.partial(kernel, n, teams),
            out_shape=(
                final, final, final,
                jax.ShapeDtypeStruct((chunks, 1, inner), f32),
                jax.ShapeDtypeStruct((teams * columns, n * depth), bf16),
                pieces,
            ),
            in_specs=[hbm, hbm, hbm, vmem, vmem],
            out_specs=(hbm, hbm, hbm, vmem, vmem, hbm),
            scratch_shapes=[
                pltpu.VMEM((PAIR, depth, inner), f32),
                pltpu.VMEM((PAIR, inner, depth), f32),
                pltpu.VMEM((PAIR, depth, inner), f32),
                pltpu.VMEM((PAIR, inner, depth), f32),
                pltpu.VMEM((inner, depth), f32),
                pltpu.VMEM((inner, LANES), f32),
                pltpu.VMEM((chunks, n, block, depth), bf16),
                pltpu.VMEM((chunks, 1, inner), f32),
                pltpu.VMEM((steps, groups, 1, inner), f32),
                pltpu.VMEM((steps, groups, 1, inner), f32),
                pltpu.VMEM((columns, depth), bf16),
                pltpu.VMEM((teams * columns, n * depth), bf16),
                dma, dma,
                dma((steps, groups)), dma((steps, groups)),
                dma((5,)), dma((5,)), dma((3,)), dma((4,)), dma,
                pltpu.VMEM((n, LEAD * PAIR, 1, inner), f32), dma, dma((2,)), dma((2,)), pltpu.SemaphoreType.REGULAR,
            ],
            compiler_params=pltpu.CompilerParams(
                collective_id=0, has_side_effects=True, vmem_limit_bytes=62 * 1024 * 1024
            ),
        )(master_gate, master_up, master_down, router_weight.T, router_gain[None, :])
        mine = lax.dynamic_slice_in_dim(
            scales.reshape(3, experts, inner), lax.axis_index("shard") * block, block, axis=2
        )
        gate, up, down, router, token = pl.pallas_call(
            place,
            out_shape=(
                final, final, final,
                jax.ShapeDtypeStruct(router.shape, bf16),
                jax.ShapeDtypeStruct((8, LANES), f32),
            ),
            in_specs=[hbm, hbm, hbm, hbm],
            out_specs=(hbm, hbm, hbm, hbm, vmem),
            scratch_shapes=[
                pltpu.VMEM((chunks, block, n * depth), bf16),
                pltpu.VMEM(router.shape, bf16),
                dma((chunks,)), dma((3,)), dma,
            ],
            compiler_params=pltpu.CompilerParams(vmem_limit_bytes=62 * 1024 * 1024),
        )(gate, up, down, router)
        token, scale_gate, scale_up, scale_down = lax.optimization_barrier((token, mine[0], mine[1], mine[2]))
        late = pl.pallas_call(
            functools.partial(finish, n),
            out_shape=pieces,
            in_specs=[hbm, hbm],
            out_specs=hbm,
            scratch_shapes=[dma, dma],
            compiler_params=pltpu.CompilerParams(
                collective_id=1, has_side_effects=True, vmem_limit_bytes=62 * 1024 * 1024
            ),
        )(later, token)
        down = pl.pallas_call(
            functools.partial(patch, n),
            out_shape=final,
            in_specs=[hbm, hbm],
            out_specs=hbm,
            scratch_shapes=[pltpu.VMEM(pieces.shape, bf16), dma((held, others)), dma],
            input_output_aliases={1: 0},
            compiler_params=pltpu.CompilerParams(vmem_limit_bytes=62 * 1024 * 1024),
        )(late, down)
        return (gate.swapaxes(1, 2), up.swapaxes(1, 2), down, scale_gate, scale_up, scale_down, router.T)

    return jax.shard_map(
        body,
        mesh=mesh,
        in_specs=(
            P("expert", "shard", None),
            P("expert", "shard", None),
            P("expert", None, "shard"),
            P("shard", "expert"),
            P("shard"),
        ),
        out_specs=(
            P("expert", None, "shard"),
            P("expert", None, "shard"),
            P("expert", "shard", None),
            P("expert", "shard"),
            P("expert", "shard"),
            P("expert", "shard"),
            P(),
        ),
        check_vma=False,
    )
```

```python
import functools

import jax
import jax.numpy as jnp
from jax import lax
from jax.experimental import pallas as pl
from jax.experimental.pallas import tpu as pltpu
from jax.sharding import PartitionSpec as P

MESH = pl.DeviceIdType.MESH
LANES = 128
PAIR = 2
CORES = 2
HELD_SHARE = 5
EARLY = 2
LEAD = 2


def across(n, me):
    half = n // 2
    return [(1 - me // half) * half + lax.rem(me, CORES) + CORES * q for q in range(half // CORES)]


def other(me, offset):
    for bit in range(offset.bit_length()):
        if offset >> bit & 1:
            me = me + (1 - 2 * lax.rem(me // 2**bit, 2)) * 2**bit
    return me


def kernel(
    n, groups_of_experts, gate, up, down, weight, gain,
    out_gate, out_up, out_down, scales, router, later,
    wide_max, tall_max, wide, tall, turned, column, stage, local, got, kept, part, rows,
    load_max, load_bulk, msg_send, msg_recv, bulk_send, bulk_recv, own_sem, router_sem, later_sem,
    first, first_load, first_send, first_recv, turn,
):
    me = lax.axis_index("shard")
    team = lax.axis_index("expert")
    experts, depth, inner = gate.shape
    block = inner // n
    per_array = experts // PAIR
    total = 3 * per_array
    direct = LEAD * PAIR
    wide_groups = 2 * per_array
    bits = n.bit_length() - 1
    cross, share, last = bits - 1, bits, bits + 1
    steps = bits + 2
    ins, outs = (gate, up, down), (out_gate, out_up, out_down)
    core = lax.rem(me, CORES)
    half = n // 2
    held = later.shape[0]
    first_held = 3 * experts - held

    def partner(step):
        size = {share: CORES, last: 1}.get(step, 2**step)
        return me + (1 - 2 * lax.rem(me // size, 2)) * size

    far, near = list(range(half, n)), list(range(CORES, half))
    orders = (far + near + [1, 0], near + far + [1, 0])

    def crosses(group):
        return lax.rem(me // CORES, 2) == lax.rem(group, 2)

    barrier = pltpu.get_barrier_semaphore()
    for d in range(1, n):
        pl.semaphore_signal(barrier, inc=1, device_id={"shard": lax.rem(me + d, n)}, device_id_type=MESH)
    for d in range(1, groups_of_experts):
        pl.semaphore_signal(
            barrier, inc=1, device_id={"expert": lax.rem(team + d, groups_of_experts)}, device_id_type=MESH
        )

    def load(group, wide_buf, tall_buf, sem, act):
        for m in range(3):

            @pl.when(group // per_array == m)
            def _():
                first = lax.rem(group, per_array) * PAIR
                act(pltpu.make_async_copy(ins[m].at[pl.ds(first, PAIR)], tall_buf if m == 2 else wide_buf, sem))

    def load_first(part, sem):
        return pltpu.make_async_copy(gate.at[part], wide.at[part], sem)

    head, rest = pl.ds(0, 1), pl.ds(1, PAIR - 1)
    load_first(head, load_bulk).start()
    load_first(rest, first_load).start()
    load(1, wide_max, tall_max, load_max, lambda c: c.start())

    def first_max(source, j, chunk):
        for b in range(inner // LANES):
            lanes = pl.ds(b * LANES, LANES)
            first[me, chunk, :, lanes] = jnp.max(jnp.abs(source[j, :, lanes]), axis=0, keepdims=True)

    def first_message(k, d):
        own = first.at[me, pl.ds(k, 1 if k == 0 else direct - 1)]
        return pltpu.make_async_remote_copy(
            own, own, first_send.at[k], first_recv.at[k],
            device_id={"shard": lax.rem(me + d, n)}, device_id_type=MESH,
        )

    def first_bytes(k):
        return first.at[pl.ds(0, n - 1), pl.ds(k, 1 if k == 0 else direct - 1)]

    load_first(head, load_bulk).wait()
    first_max(wide, 0, 0)
    pl.semaphore_wait(barrier, n + groups_of_experts - 2)
    for d in range(1, n):
        first_message(0, d).start()
    load_first(rest, first_load).wait()
    for j in range(1, PAIR):
        first_max(wide, j, j)
    load(1, wide_max, tall_max, load_max, lambda c: c.wait())
    for j in range(PAIR):
        first_max(wide_max, j, PAIR + j)
    load(LEAD, wide_max, tall_max, load_max, lambda c: c.start())
    for d in range(1, n):
        first_message(1, d).start()

    team_rows = pl.ds(pl.multiple_of(team * part.shape[0], part.shape[0]), part.shape[0])
    my_columns = pl.ds(pl.multiple_of(me * depth, depth), depth)
    product = (weight[...] * gain[...]).astype(jnp.bfloat16)
    part[...] = product
    rows[team_rows, my_columns] = product
    for d in range(1, n):
        pltpu.make_async_remote_copy(
            part, rows.at[team_rows, my_columns], router_sem.at[0], router_sem.at[1],
            device_id={"shard": lax.rem(me + d, n)}, device_id_type=MESH,
        ).start()
    router_bytes = rows.at[pl.ds(0, part.shape[0]), pl.ds(0, (n - 1) * depth)]
    team_bytes = rows.at[pl.ds(0, (groups_of_experts - 1) * part.shape[0])]

    def message(step, group):
        source = local.at[group * PAIR + 1 - core] if step == 0 else kept.at[step, group]
        return pltpu.make_async_remote_copy(
            source, got.at[step, group], msg_send.at[step, group], msg_recv.at[step, group],
            device_id={"shard": partner(step)}, device_id_type=MESH,
        )

    def local_max(group):
        load(group, wide_max, tall_max, load_max, lambda c: c.wait())

        @pl.when(group < wide_groups)
        def _():
            for j in range(PAIR):
                for b in range(inner // LANES):
                    lanes = pl.ds(b * LANES, LANES)
                    local[group * PAIR + j, :, lanes] = jnp.max(jnp.abs(wide_max[j, :, lanes]), axis=0, keepdims=True)

        @pl.when(group >= wide_groups)
        def _():
            for j in range(PAIR):
                for b in range(inner // LANES):
                    lanes = pl.ds(b * LANES, LANES)
                    most = jnp.abs(tall_max[j, lanes, pl.ds(0, LANES)])
                    for h in range(1, depth // LANES):
                        most = jnp.maximum(most, jnp.abs(tall_max[j, lanes, pl.ds(h * LANES, LANES)]))
                    local[group * PAIR + j, :, lanes] = jnp.max(most.T, axis=0, keepdims=True)

        @pl.when(group + 1 < total)
        def _():
            load(group + 1, wide_max, tall_max, load_max, lambda c: c.start())

        message(0, group).start()

    def reduce_step(step, group):
        if step < share:
            message(step - 1, group).wait_recv()
            held = local[group * PAIR + core] if step == 1 else kept[step - 1, group]
            kept[step, group] = jnp.maximum(held, got[step - 1, group])
            if step < cross:
                message(step, group).start()
                return

        @pl.when(crosses(group))
        def _():
            if step == share:
                message(cross, group).wait_recv()
                kept[share, group] = jnp.maximum(kept[cross, group], got[cross, group])
            if step == last:
                kept[last, group] = kept[share, group]
            else:
                message(step, group).start()

        if step == last:

            @pl.when(jnp.logical_not(crosses(group)))
            def _():
                message(share, group).wait_recv()
                kept[last, group] = got[share, group]

            scales[group * PAIR + core] = kept[last, group]
            message(last, group).start()

    def normalise(j, source, chunk, p):
        part_rows = pl.ds(p * block if isinstance(p, int) else pl.multiple_of(p * block, 8), block)
        for h in range(depth // LANES):
            lanes = pl.ds(h * LANES, LANES)
            x = source[part_rows, lanes] if j is None else source[j, part_rows, lanes]
            stage[chunk, p, :, lanes] = (x / column[part_rows]).astype(jnp.bfloat16)

    def spread(chunk):
        for b in range(inner // LANES):
            lanes = pl.ds(b * LANES, LANES)
            column[lanes] = jnp.broadcast_to(scales[chunk, :, lanes], (LANES, LANES)).T

    def turn_over(j):
        for b in range(inner // LANES):
            lanes = pl.ds(b * LANES, LANES)
            for h in range(depth // LANES):
                part = pl.ds(h * LANES, LANES)
                turned[lanes, part] = wide[j, part, lanes].T

    def keep(chunk, m):
        pltpu.make_async_copy(
            stage.at[chunk, me], outs[m].at[chunk - m * experts, :, my_columns], own_sem.at[m]
        ).start()

    def first_bulk(chunk):
        j = lax.rem(chunk, PAIR)

        @pl.when((chunk > 0) & (j == 0))
        def _():
            load(chunk // PAIR, wide, tall, load_bulk, lambda c: c.wait())

        @pl.when(chunk > 0)
        def _():
            turn_over(j)

        for k in range(2):

            @pl.when(chunk == k)
            def _():
                pltpu.make_async_copy(first_bytes(k), first_bytes(k), first_recv.at[k]).wait()

        for b in range(inner // LANES):
            lanes = pl.ds(b * LANES, LANES)
            scales[chunk, :, lanes] = jnp.max(first[:, chunk, :, lanes], axis=0)
        spread(chunk)
        for c in range(CORES):

            @pl.when(core == c)
            def _():
                for offset in orders[c]:
                    p = other(me, offset)
                    normalise(None, turned, chunk, p)
                    if offset == 0:
                        keep(chunk, 0)
                    else:
                        send(chunk, p, 0)

        @pl.when(j == PAIR - 1)
        def _():
            load((chunk + 1) // PAIR, wide, tall, load_bulk, lambda c: c.start())

    def send(chunk, p, m):
        s = m
        if m == 2:
            s = jnp.where(chunk >= first_held, jnp.where(chunk == 3 * experts - 1, 4, 3), 2)
        pltpu.make_async_remote_copy(
            stage.at[chunk, p], outs[m].at[chunk - m * experts, :, my_columns], bulk_send.at[s], bulk_recv.at[s],
            device_id={"shard": p}, device_id_type=MESH,
        ).start()

    def deal(chunk, offset, m, c):
        p = other(me, offset)
        if offset == 0:
            keep(chunk, m)
        elif m < 2 or offset < half or offset % CORES:
            send(chunk, p, m)
        else:

            @pl.when(chunk < first_held)
            def _():
                send(chunk, p, m)

            if c == 0:

                @pl.when(chunk >= first_held)
                def _():
                    pltpu.make_async_copy(
                        stage.at[chunk, p], later.at[chunk - first_held, lax.rem(p, half) // CORES], later_sem
                    ).start()

    def bulk(group):
        message(last, group).wait_recv()
        scales[group * PAIR + 1 - core] = got[last, group]

        load(group, wide, tall, load_bulk, lambda c: c.wait())

        @pl.loop(0, PAIR)
        def _(j):
            chunk = group * PAIR + j
            spread(chunk)

            @pl.when(group < wide_groups)
            def _():
                turn_over(j)
                for p in range(n):
                    normalise(None, turned, chunk, p)

            @pl.when(group >= wide_groups)
            def _():
                for p in range(n):
                    normalise(j, tall, chunk, p)

            for m in range(3):

                @pl.when(group // per_array == m)
                def _():
                    for c in range(CORES):

                        @pl.when(core == c)
                        def _():
                            for offset in orders[c]:
                                deal(chunk, offset, m, c)

        @pl.when(group + 1 < total)
        def _():
            load(group + 1, wide, tall, load_bulk, lambda c: c.start())

    turn_over(0)

    @pl.loop(LEAD, total + steps)
    def _(t):
        for step in reversed(range(1, steps)):

            @pl.when((t >= step + LEAD) & (t < total + step))
            def _():
                reduce_step(step, t - step)

        @pl.when((t > LEAD) & (t <= LEAD + direct))
        def _():
            first_bulk(t - LEAD - 1)

        @pl.when(t < total)
        def _():
            local_max(t)

        @pl.when(t == LEAD + 1)
        def _():
            pltpu.make_async_copy(router_bytes, router_bytes, router_sem.at[1]).wait()
            for d in range(1, groups_of_experts):
                pltpu.make_async_remote_copy(
                    rows.at[team_rows], rows.at[team_rows], router_sem.at[2], router_sem.at[3],
                    device_id={"expert": lax.rem(team + d, groups_of_experts)}, device_id_type=MESH,
                ).start()

        @pl.when(t >= LEAD + steps)
        def _():
            bulk(t - steps)

    def done(sems, s, m, count, width):
        moved = outs[m].at[pl.ds(0, count), :, pl.ds(0, width * depth)]
        pltpu.make_async_copy(moved, moved, sems.at[s]).wait()

    def done_first(sems, narrow):
        for m in range(3):
            done(sems, m, m, experts - held if m == 2 else experts, n - 1)
        done(sems, 3, 2, held - 1, n - 1 - narrow)

    @pl.when(core == 0)
    def _():
        done_first(bulk_send, half // CORES)
        done(bulk_send, 4, 2, 1, n - 1 - half // CORES)
        for q in range(half // CORES):
            pl.semaphore_signal(
                turn, inc=1, device_id={"shard": me // half * half + CORES * q + 1}, device_id_type=MESH
            )

    @pl.when(core > 0)
    def _():
        def send_held(chunk):
            for p in across(n, me):
                send(chunk, p, 2)

        pl.loop(first_held, first_held + EARLY)(send_held)
        pl.semaphore_wait(turn, half // CORES)
        pl.loop(first_held + EARLY, 3 * experts)(send_held)

    pltpu.make_async_copy(router_bytes, router_bytes, router_sem.at[0]).wait()
    for s in (2, 3):
        pltpu.make_async_copy(team_bytes, team_bytes, router_sem.at[s]).wait()
    router[...] = rows[...]

    @pl.loop(LEAD, total)
    def _(group):
        for step in range(steps):
            if step in (cross, share):

                @pl.when(crosses(group))
                def _():
                    message(step, group).wait_send()
            else:
                message(step, group).wait_send()

    for k in range(2):
        pltpu.make_async_copy(first_bytes(k), first_bytes(k), first_send.at[k]).wait()

    for m in range(3):
        own = outs[m].at[:, :, pl.ds(0, depth)]
        pltpu.make_async_copy(own, own, own_sem.at[m]).wait()

    @pl.when(core == 0)
    def _():
        pltpu.make_async_copy(later, later, later_sem).wait()
        done_first(bulk_recv, half // CORES)
        done(bulk_recv, 4, 2, 1, n - 1 - half // CORES)

    @pl.when(core > 0)
    def _():
        for sems in (bulk_send, bulk_recv):
            done_first(sems, 0)
            done(sems, 4, 2, 1, n - 1)


def place(
    gate, up, down, router, out_gate, out_up, out_down, out_router, token,
    buffer, router_buffer, loads, stores, router_sem,
):
    ins, outs = (gate, up, down), (out_gate, out_up, out_down)
    experts = gate.shape[0]

    def load(m, e):
        chunk = m * experts + e
        return pltpu.make_async_copy(ins[m].at[e], buffer.at[chunk], loads.at[chunk])

    for m in range(3):

        @pl.loop(0, experts)
        def _(e):
            load(m, e).start()

    pltpu.make_async_copy(router, router_buffer, router_sem).start()
    for m in range(3):

        @pl.loop(0, experts)
        def _(e):
            load(m, e).wait()
            pltpu.make_async_copy(buffer.at[m * experts + e], outs[m].at[e], stores.at[m]).start()

    pltpu.make_async_copy(router, router_buffer, router_sem).wait()
    pltpu.make_async_copy(router_buffer, out_router, router_sem).start()
    token[...] = jnp.zeros_like(token)
    for m in range(3):
        pltpu.make_async_copy(outs[m], outs[m], stores.at[m]).wait()
    pltpu.make_async_copy(router_buffer, out_router, router_sem).wait()


def finish(n, later, token, late, send_sem, recv_sem):
    me = lax.axis_index("shard")
    held, others = later.shape[:2]

    @pl.when(lax.rem(me, CORES) == 0)
    def _():
        barrier = pltpu.get_barrier_semaphore()
        for p in across(n, me):
            pl.semaphore_signal(barrier, inc=1, device_id={"shard": p}, device_id_type=MESH)
        pl.semaphore_wait(barrier, others)

        @pl.loop(0, held)
        def _(i):
            for q, p in enumerate(across(n, me)):
                pltpu.make_async_remote_copy(
                    later.at[i, q], late.at[i, lax.rem(me, n // 2) // CORES], send_sem, recv_sem,
                    device_id={"shard": p}, device_id_type=MESH,
                ).start()

        pltpu.make_async_copy(late, late, send_sem).wait()
        pltpu.make_async_copy(late, late, recv_sem).wait()


def patch(n, late, down, out_down, store):
    me = lax.axis_index("shard")
    held, others, block, depth = late.shape
    first = down.shape[0] - held

    @pl.when(lax.rem(me, CORES) == 0)
    def _():
        for i in range(held):
            for q, p in enumerate(across(n, me)):
                columns = pl.ds(pl.multiple_of(p * depth, depth), depth)
                pltpu.make_async_copy(late.at[i, q], out_down.at[first + i, :, columns], store).start()
        pltpu.make_async_copy(late, late, store).wait()


def plain(master_gate, master_up, master_down, router_weight, router_gain):
    scale_gate, scale_up, scale_down = lax.pmax(
        (
            jnp.max(jnp.abs(master_gate), axis=1),
            jnp.max(jnp.abs(master_up), axis=1),
            jnp.max(jnp.abs(master_down), axis=2),
        ),
        "shard",
    )
    narrow_gate, narrow_up, narrow_down = (
        (master_gate / jnp.expand_dims(scale_gate, 1)).astype(jnp.bfloat16),
        (master_up / jnp.expand_dims(scale_up, 1)).astype(jnp.bfloat16),
        (master_down / jnp.expand_dims(scale_down, 2)).astype(jnp.bfloat16),
    )
    final_gate, final_up = (
        lax.all_to_all(narrow_gate, "shard", split_axis=2, concat_axis=1, tiled=True),
        lax.all_to_all(narrow_up, "shard", split_axis=2, concat_axis=1, tiled=True),
    )
    final_down = lax.all_to_all(narrow_down, "shard", split_axis=1, concat_axis=2, tiled=True)
    scale_gate = lax.dynamic_slice_in_dim(
        scale_gate, lax.axis_index("shard") * final_gate.shape[2], final_gate.shape[2], axis=1
    )
    scale_up = lax.dynamic_slice_in_dim(
        scale_up, lax.axis_index("shard") * final_up.shape[2], final_up.shape[2], axis=1
    )
    scale_down = lax.dynamic_slice_in_dim(
        scale_down, lax.axis_index("shard") * final_down.shape[1], final_down.shape[1], axis=1
    )
    part_router = (router_weight * router_gain[:, None]).astype(jnp.bfloat16)
    row_router = lax.all_gather(part_router, "shard", axis=0, tiled=True)
    serve_router = lax.all_gather(row_router, "expert", axis=1, tiled=True)
    return (final_gate, final_up, final_down, scale_gate, scale_up, scale_down, serve_router)


def solution(mesh):
    n, teams = mesh.shape["shard"], mesh.shape["expert"]

    def body(master_gate, master_up, master_down, router_weight, router_gain):
        experts, depth, inner = master_gate.shape
        block = inner // n
        chunks = 3 * experts
        groups = chunks // PAIR
        steps = n.bit_length() + 1
        columns = router_weight.shape[1]
        fits = depth % LANES == 0 and inner % LANES == 0 and block % 8 == 0
        if n < 8 or n & (n - 1) or experts < (LEAD + 1) * PAIR or experts % PAIR or not fits:
            return plain(master_gate, master_up, master_down, router_weight, router_gain)
        f32, bf16 = jnp.float32, jnp.bfloat16
        dma = pltpu.SemaphoreType.DMA
        final = jax.ShapeDtypeStruct((experts, block, n * depth), bf16)
        hbm, vmem = pl.BlockSpec(memory_space=pl.ANY), pl.BlockSpec(memory_space=pltpu.VMEM)
        held = chunks // HELD_SHARE
        others = n // 2 // CORES
        pieces = jax.ShapeDtypeStruct((held, others, block, depth), bf16)
        gate, up, down, scales, router, later = pl.pallas_call(
            functools.partial(kernel, n, teams),
            out_shape=(
                final, final, final,
                jax.ShapeDtypeStruct((chunks, 1, inner), f32),
                jax.ShapeDtypeStruct((teams * columns, n * depth), bf16),
                pieces,
            ),
            in_specs=[hbm, hbm, hbm, vmem, vmem],
            out_specs=(hbm, hbm, hbm, vmem, vmem, hbm),
            scratch_shapes=[
                pltpu.VMEM((PAIR, depth, inner), f32),
                pltpu.VMEM((PAIR, inner, depth), f32),
                pltpu.VMEM((PAIR, depth, inner), f32),
                pltpu.VMEM((PAIR, inner, depth), f32),
                pltpu.VMEM((inner, depth), f32),
                pltpu.VMEM((inner, LANES), f32),
                pltpu.VMEM((chunks, n, block, depth), bf16),
                pltpu.VMEM((chunks, 1, inner), f32),
                pltpu.VMEM((steps, groups, 1, inner), f32),
                pltpu.VMEM((steps, groups, 1, inner), f32),
                pltpu.VMEM((columns, depth), bf16),
                pltpu.VMEM((teams * columns, n * depth), bf16),
                dma, dma,
                dma((steps, groups)), dma((steps, groups)),
                dma((5,)), dma((5,)), dma((3,)), dma((4,)), dma,
                pltpu.VMEM((n, LEAD * PAIR, 1, inner), f32), dma, dma((2,)), dma((2,)), pltpu.SemaphoreType.REGULAR,
            ],
            compiler_params=pltpu.CompilerParams(
                collective_id=0, has_side_effects=True, vmem_limit_bytes=62 * 1024 * 1024
            ),
        )(master_gate, master_up, master_down, router_weight.T, router_gain[None, :])
        mine = lax.dynamic_slice_in_dim(
            scales.reshape(3, experts, inner), lax.axis_index("shard") * block, block, axis=2
        )
        gate, up, down, router, token = pl.pallas_call(
            place,
            out_shape=(
                final, final, final,
                jax.ShapeDtypeStruct(router.shape, bf16),
                jax.ShapeDtypeStruct((8, LANES), f32),
            ),
            in_specs=[hbm, hbm, hbm, hbm],
            out_specs=(hbm, hbm, hbm, hbm, vmem),
            scratch_shapes=[
                pltpu.VMEM((chunks, block, n * depth), bf16),
                pltpu.VMEM(router.shape, bf16),
                dma((chunks,)), dma((3,)), dma,
            ],
            compiler_params=pltpu.CompilerParams(vmem_limit_bytes=62 * 1024 * 1024),
        )(gate, up, down, router)
        token, scale_gate, scale_up, scale_down = lax.optimization_barrier((token, mine[0], mine[1], mine[2]))
        late = pl.pallas_call(
            functools.partial(finish, n),
            out_shape=pltpu.VMEM(pieces.shape, bf16),
            in_specs=[hbm, hbm],
            out_specs=vmem,
            scratch_shapes=[dma, dma],
            compiler_params=pltpu.CompilerParams(
                collective_id=1, has_side_effects=True, vmem_limit_bytes=16 * 1024 * 1024
            ),
        )(later, token)
        down = pl.pallas_call(
            functools.partial(patch, n),
            out_shape=final,
            in_specs=[vmem, hbm],
            out_specs=hbm,
            scratch_shapes=[dma],
            input_output_aliases={1: 0},
            compiler_params=pltpu.CompilerParams(vmem_limit_bytes=16 * 1024 * 1024),
        )(pltpu.with_memory_space_constraint(late, pltpu.VMEM), down)
        return (gate.swapaxes(1, 2), up.swapaxes(1, 2), down, scale_gate, scale_up, scale_down, router.T)

    return jax.shard_map(
        body,
        mesh=mesh,
        in_specs=(
            P("expert", "shard", None),
            P("expert", "shard", None),
            P("expert", None, "shard"),
            P("shard", "expert"),
            P("shard"),
        ),
        out_specs=(
            P("expert", None, "shard"),
            P("expert", None, "shard"),
            P("expert", "shard", None),
            P("expert", "shard"),
            P("expert", "shard"),
            P("expert", "shard"),
            P(),
        ),
        check_vma=False,
    )
```
